256 devices in a mesh: zero: 16 (over y, x), model: 8 (over z), copy: 2 (over core).
Axes of the slice: x: 4, y: 4, z: 8, core: 2. Of those that a mesh axis runs over, the one named last changes fastest.
Arguments:
- train_query: float32 [10240, 5120], P(('copy', 'zero'), 'model'), parts along dimension 0, may hold values from -0.125 to 0.125
- slow_query: float32 [10240, 5120], P(('copy', 'zero'), 'model'), parts along dimension 0, may hold values from -0.078125 to 0.078125
- train_key: float32 [10240, 5120], P(('copy', 'zero'), 'model'), parts along dimension 0, may hold values from -0.125 to 0.125
- slow_key: float32 [10240, 5120], P(('copy', 'zero'), 'model'), parts along dimension 0, may hold values from -0.078125 to 0.078125
- train_value: float32 [10240, 5120], P(('copy', 'zero'), 'model'), parts along dimension 0, may hold values from -0.125 to 0.125
- slow_value: float32 [10240, 5120], P(('copy', 'zero'), 'model'), parts along dimension 0, may hold values from -0.078125 to 0.078125
- norm_train: float32 [10240], P(('copy', 'zero', 'model')), parts along dimension 0, may hold values from 0.25 to 1.75
- norm_step: float32 [10240], P(('copy', 'zero', 'model')), parts along dimension 0, may hold values from -0.3 to 0.3
Outputs:
- final_query: bfloat16 [10240, 5120], P('copy', 'model'), parts along dimension 0
- final_key: bfloat16 [10240, 5120], P('copy', 'model'), parts along dimension 0
- final_value: bfloat16 [10240, 5120], P('copy', 'model'), parts along dimension 0
- scale_query: float32 [10240], P(('copy', 'model')), parts along dimension 0
- scale_key: float32 [10240], P(('copy', 'model')), parts along dimension 0
- scale_value: float32 [10240], P(('copy', 'model')), parts along dimension 0
- serve_norm: bfloat16 [10240], P('copy'), parts along dimension 0
- result_query: float32 [10240, 5120], P(('copy', 'zero'), 'model'), parts along dimension 0
- result_key: float32 [10240, 5120], P(('copy', 'zero'), 'model'), parts along dimension 0
- result_value: float32 [10240, 5120], P(('copy', 'zero'), 'model'), parts along dimension 0
The draws below stay inside these ranges and needn't reach their ends.
There are 2 independent parts, one for each index of `copy`. The reference program is written for one: setup_inputs(seed, part) draws one part's arguments, and reference() takes and returns one part's arrays. A program takes and returns all parts, laid end to end along the dimension named above; each array names one. Nothing has to cross between parts.
All inputs are finite; a program needn't handle non-finite values.
Results may differ from the reference program's by a relative error of at most 0.001.
Values may be sent and summed in bfloat16 or wider, within the bound.
A program may use at most 128 MiB of HBM per device.

```python
import jax
import jax.numpy as jnp
from jax import lax

D_MODEL = 5120
Q_DIM = 5120
KV_DIM = 5120


def strengthened(array, stream_key, source, target, parts, factor):
    owner, partner = [(jnp.arange(array.shape[axis_at]) // (array.shape[axis_at] // parts)).reshape([-1 if axis == axis_at else 1 for axis in range(array.ndim)]) for axis_at in (source, target)]
    chosen = jax.random.permutation(stream_key, parts)[partner]
    strong = (owner == chosen) | (owner == (partner + parts // 2) % parts)
    return jnp.where(strong, factor * array, array)


def block_levels(stream_key, dims, pieces, low, top_value):
    factor_of, own = 1.0, jax.random.fold_in(stream_key, 6)
    for position, blocks in pieces:
        heights = jnp.exp(jax.random.uniform(jax.random.fold_in(own, position), (blocks,), jnp.float32, low / len(pieces), top_value / len(pieces)))
        factor_of = factor_of * jnp.repeat(heights, dims[position] // blocks).reshape([-1 if axis == position else 1 for axis in range(len(dims))])
    return factor_of


def normal_values(stream_key, dims, deviation, reach, shards=(), dtype=jnp.bfloat16):
    entries = jax.random.normal(stream_key, dims, jnp.float32) * deviation
    if len(shards) > 0:
        entries = block_levels(stream_key, dims, shards, -0.22, 0.18) * entries
    return jnp.clip(entries, min=-reach, max=reach).astype(dtype)


def bell_draw_with(own_key, shape, scale, bound, split, heavy, kind=jnp.bfloat16):
    drawn = scale * jax.random.normal(own_key, shape, jnp.float32)
    if split:
        drawn = drawn * block_levels(own_key, shape, split, -0.22, 0.18)
    return jnp.clip(strengthened(drawn, jax.random.fold_in(own_key, 3), *heavy), -bound, bound).astype(kind)


def setup_inputs(seed: int = 0, part: int = 0) -> dict:
    keys = jax.random.split(jax.random.key(seed), 9)
    part_splits = jax.random.split(jax.random.fold_in(keys[8], part), 9)
    train_query = bell_draw_with(part_splits[0], (D_MODEL, Q_DIM), D_MODEL ** -0.5, 0.125, ((0, 16), (1, 8)), (0, 1, 16, 2.0), jnp.float32)
    slow_query = normal_values(part_splits[1], (D_MODEL, Q_DIM), D_MODEL ** -0.5, 0.078125, ((0, 16), (1, 8)), jnp.float32)
    train_key = bell_draw_with(part_splits[2], (D_MODEL, KV_DIM), D_MODEL ** -0.5, 0.125, ((0, 16), (1, 8)), (0, 1, 16, 2.0), jnp.float32)
    slow_key = normal_values(part_splits[3], (D_MODEL, KV_DIM), D_MODEL ** -0.5, 0.078125, ((0, 16), (1, 8)), jnp.float32)
    train_value = bell_draw_with(part_splits[4], (D_MODEL, KV_DIM), D_MODEL ** -0.5, 0.125, ((0, 16), (1, 8)), (0, 1, 16, 2.0), jnp.float32)
    slow_value = normal_values(part_splits[5], (D_MODEL, KV_DIM), D_MODEL ** -0.5, 0.078125, ((0, 16), (1, 8)), jnp.float32)
    norm_train = jnp.clip(1.0 + 0.15 * jax.random.normal(part_splits[6], (D_MODEL,), jnp.float32), 0.25, 1.75)
    norm_step = jnp.clip(jax.random.uniform(part_splits[7], (D_MODEL,), jnp.float32, -0.3, 0.3) * block_levels(part_splits[7], (D_MODEL,), ((0, 128),), -0.4, 0.0), -0.3, 0.3)
    return {"train_query": train_query, "slow_query": slow_query, "train_key": train_key, "slow_key": slow_key, "train_value": train_value, "slow_value": slow_value, "norm_train": norm_train, "norm_step": norm_step}


keep_rate = 0.75

def reference(train_query, slow_query, train_key, slow_key, train_value, slow_value, norm_train, norm_step):
    result_query = keep_rate * slow_query + (1.0 - keep_rate) * train_query
    result_key = keep_rate * slow_key + (1.0 - keep_rate) * train_key
    result_value = keep_rate * slow_value + (1.0 - keep_rate) * train_value
    scale_query = jnp.sqrt(lax.optimization_barrier(jnp.sum(result_query * result_query, axis=0)))
    final_query = (result_query / scale_query).astype(jnp.bfloat16)
    scale_key = jnp.sqrt(lax.optimization_barrier(jnp.sum(result_key * result_key, axis=0)))
    final_key = (result_key / scale_key).astype(jnp.bfloat16)
    scale_value = jnp.sqrt(lax.optimization_barrier(jnp.sum(result_value * result_value, axis=0)))
    final_value = (result_value / scale_value).astype(jnp.bfloat16)
    serve_norm = (norm_train + norm_step).astype(jnp.bfloat16)
    return (final_query, final_key, final_value, scale_query, scale_key, scale_value, serve_norm, result_query, result_key, result_value)
```

```python
import functools

import jax
import jax.numpy as jnp
from jax import lax
from jax.experimental import pallas as pl
from jax.experimental.pallas import tpu as pltpu
from jax.sharding import Mesh
from jax.sharding import PartitionSpec as P

COPY_ZERO = ("copy", "zero_0", "zero_1")
COPY_ZERO_MODEL = ("copy", "zero_0", "zero_1", "model")
MESH = pl.DeviceIdType.MESH

KEEP_RATE = 0.75
SIDE = 4
PLANE = SIDE * SIDE
DEPTH = 8
LINKS = (("zero_1", 1), ("zero_1", -1), ("zero_0", 1), ("zero_0", -1))
WINDOW = 384
EARLY = {"zero_1": (8, 32), "zero_0": (24, 16)}


ORDER = (
    ("own 1", None), ("own 0", None), ("side 1", 0), ("pass", None), ("side 1", -1), ("side 1", 1), ("side 1", 2),
    ("side 0", None), ("side pass", None),
)
FIRST = 3
NEXT = {0: 3, 1: 4, 2: 5, 3: 6, 4: 7, 6: 8}


def place(here, link, kind, across, arrived):
    axis, step = LINKS[link]
    along = (-step if "pass" in kind else 0) - (step if arrived else 0)
    at = lax.rem(here[axis] + along + 2 * SIDE, SIDE)
    if "side" in kind:
        unit = link ^ 2 if kind != "side 0" else link ^ 3
        other = "zero_0" if axis == "zero_1" else "zero_1"
        beside = slice(None) if across is None else lax.rem(here[other] + across + SIDE, SIDE)
        return (beside, at, unit) if axis == "zero_1" else (at, beside, unit)
    unit = link ^ 1 if kind == "own 0" else link
    return (here["zero_0"], at, unit) if axis == "zero_1" else (at, here["zero_1"], unit)


def work(
    train_q, slow_q, train_k, slow_k, train_v, slow_v, gain_train, gain_step,
    out, result, scale_q, scale_k, scale_v, gain,
    train, slow, early, sums_x, sums_y, gains, gain_z, gain_plane, gain_rows,
    load_sem, gain_sem, early_send, early_recv, sum_send, sum_recv, z_send, z_recv, plane_send, plane_recv,
    link_send, link_recv, ready,
):
    rows, width = train_q.shape
    unit = rows // 4
    columns = [slice(w * width, (w + 1) * width) for w in range(3)]
    x, y, z = lax.axis_index("zero_1"), lax.axis_index("zero_0"), lax.axis_index("model")
    me = y * SIDE + x
    here = {"zero_1": x, "zero_0": y}

    def near(axis, step):
        return {axis: lax.rem(here[axis] + step + SIDE, SIDE)}

    def deep(step):
        return lax.rem(z + step + DEPTH, DEPTH)

    barrier = pltpu.get_barrier_semaphore()
    friends = [near(axis, step) for axis in ("zero_1", "zero_0") for step in (1, 2, 3)]
    for friend in friends:
        pl.semaphore_signal(barrier, inc=1, device_id=friend, device_id_type=MESH)

    top = DEPTH - 1
    lower = (z + top) // DEPTH + (z + 1) // DEPTH

    def greet(sem, step):
        pl.semaphore_signal(sem, inc=1, device_id={"model": deep(step)}, device_id_type=MESH)

    pl.when(z < top)(lambda: greet(barrier, 1))
    pl.when(z == 0)(lambda: greet(barrier, -1))

    ahead = [sum(EARLY[axis]) for axis, _ in LINKS]
    first = [EARLY[axis][0] for axis, _ in LINKS]
    spans = [(u * unit, first[u]) for u in range(4)] + [(u * unit + first[u], unit - first[u]) for u in range(4)]
    loads = []
    for n, (start, size) in enumerate(spans):
        at = pl.ds(start, size)
        group = []
        for w, (t, s) in enumerate(((train_q, slow_q), (train_k, slow_k), (train_v, slow_v))):
            group.append(pltpu.make_async_copy(t.at[at, :], train.at[at, columns[w]], load_sem.at[n, w, 0]))
            group.append(pltpu.make_async_copy(s.at[at, :], slow.at[at, columns[w]], load_sem.at[n, w, 1]))
        for c in group:
            c.start()
        loads.append(group)
    gain_loads = [
        pltpu.make_async_copy(gain_train, gains.at[0], gain_sem.at[0]),
        pltpu.make_async_copy(gain_step, gains.at[1], gain_sem.at[1]),
    ]
    for c in gain_loads:
        c.start()

    def average(n):
        for c in loads[n]:
            c.wait()
        start, size = spans[n]
        r = KEEP_RATE * slow[start : start + size, :] + (1.0 - KEEP_RATE) * train[start : start + size, :]
        result[start : start + size, :] = r
        return jnp.sum((r * r).reshape(size // 8, 8, 3 * width), axis=0)

    def early_copy(link, half):
        axis, step = LINKS[link]
        first, second = EARLY[axis]
        start, size = (0, first) if half == 0 else (first, second)
        return pltpu.make_async_remote_copy(
            src_ref=result.at[pl.ds(link * unit + start, size), :], dst_ref=early.at[link, pl.ds(start, size), :],
            send_sem=early_send.at[link, half], recv_sem=early_recv.at[link, half],
            device_id=near(axis, step), device_id_type=MESH,
        )

    square = average(0)
    for n in range(1, 4):
        square = square + average(n)
    pl.semaphore_wait(barrier, len(friends) + lower)
    for link in range(4):
        early_copy(link, 0).start()
    for n in range(4, 8):
        square = square + average(n)

    def ring(ref, index, axis, send, recv):
        copies = []
        for step in (1, 2, 3):
            copies.append(pltpu.make_async_remote_copy(
                src_ref=ref.at[index], dst_ref=ref.at[index], send_sem=send.at[step - 1], recv_sem=recv.at[step - 1],
                device_id=near(axis, step), device_id_type=MESH,
            ))
            copies[-1].start()
        return copies

    def landed(ref, axis, send, recv):
        for step in (1, 2, 3):
            index = near(axis, -step)[axis]
            pltpu.make_async_remote_copy(
                src_ref=ref.at[index], dst_ref=ref.at[index], send_sem=send.at[step - 1], recv_sem=recv.at[step - 1],
                device_id=near(axis, step), device_id_type=MESH,
            ).wait_recv()

    sums_x[x] = jnp.sum(square, axis=0, keepdims=True)
    sent = ring(sums_x, x, "zero_1", sum_send.at[0], sum_recv.at[0])
    for link in (0, 1):
        early_copy(link, 1).start()

    pl.when(z > 0)(lambda: greet(ready, -1))
    pl.when(z == top)(lambda: greet(ready, 1))

    for c in gain_loads:
        c.wait()
    value = (gains[0] + gains[1]).astype(jnp.bfloat16)
    count = gain_train.shape[1]
    put = (
        lax.broadcasted_iota(jnp.int32, (count, WINDOW), 1)
        == lax.broadcasted_iota(jnp.int32, (count, WINDOW), 0) + (lax.rem(me, 2) * 64 + z * count)
    )
    gain_z[z] = jnp.dot(value, jnp.where(put, 1.0, 0.0).astype(jnp.bfloat16), preferred_element_type=jnp.float32)

    landed(sums_x, "zero_1", sum_send.at[0], sum_recv.at[0])
    sums_y[y] = (sums_x[0] + sums_x[1]) + (sums_x[2] + sums_x[3])
    sent += ring(sums_y, y, "zero_0", sum_send.at[1], sum_recv.at[1])
    for link in (2, 3):
        early_copy(link, 1).start()
    landed(sums_y, "zero_0", sum_send.at[1], sum_recv.at[1])
    root = jnp.sqrt((sums_y[0] + sums_y[1]) + (sums_y[2] + sums_y[3]))
    inverse = 1.0 / root

    def normalise(link, start, size):
        out[y, x, link, pl.ds(start, size), :] = (
            result[link * unit + start : link * unit + start + size, :] * inverse
        ).astype(jnp.bfloat16)

    def piece(link, k, arrived):
        kind, across = ORDER[k]
        block = place(here, link, kind, across, arrived)
        start = ahead[link] if kind == "own 1" else 0
        return out.at[(*block, pl.ds(start, unit - start))]

    def copy(link, k, arrived):
        ref = piece(link, k, arrived)
        return pltpu.make_async_remote_copy(
            src_ref=ref, dst_ref=ref, send_sem=link_send.at[link, k], recv_sem=link_recv.at[link, k],
            device_id=near(*LINKS[link]), device_id_type=MESH,
        )

    for link in range(4):
        normalise(link, ahead[link], unit - ahead[link])
        copy(link, 0, False).start()
    for link in range(4):
        normalise(link, 0, ahead[link])
    for k in range(1, FIRST):
        for link in range(4):
            copy(link, k, False).start()
    for w, ref in enumerate((scale_q, scale_k, scale_v)):
        ref[...] = root[0, columns[w]]

    for link in range(4):
        axis, step = LINKS[link]
        for half in range(2):
            early_copy(link, half).wait_recv()
        at = {**here, **near(axis, -step)}
        out[at["zero_0"], at["zero_1"], link, pl.ds(0, ahead[link]), :] = (
            early[link, : ahead[link], :] * inverse
        ).astype(jnp.bfloat16)

    def hop(step, up, arrived):
        index = deep((1 - step if up else step - 1) + (0 if not arrived else -1 if up else 1))
        at = (0 if up else 4) + step - 1
        return pltpu.make_async_remote_copy(
            src_ref=gain_z.at[index], dst_ref=gain_z.at[index], send_sem=z_send.at[at], recv_sem=z_recv.at[at],
            device_id={"model": deep(1 if up else -1)}, device_id_type=MESH,
        )

    hops = [(step, up) for step in range(1, 5) for up in ((True, False) if step < 4 else (True,))]

    def gains_at(k):
        if k <= 4:
            for step, up in hops:
                if step == k:
                    hop(step, up, True).wait_recv()
            for step, up in hops:
                if step == k + 1:
                    hop(step, up, False).start()
        if k == 4:
            column = gain_z[0]
            for n in range(1, DEPTH):
                column = column + gain_z[n]
            gain_plane[y, x] = column
            return ring(gain_plane.at[y], x, "zero_1", plane_send.at[0], plane_recv.at[0])
        if k == 6:
            landed(gain_plane.at[y], "zero_1", plane_send.at[0], plane_recv.at[0])
            return ring(gain_plane, y, "zero_0", plane_send.at[1], plane_recv.at[1])
        if k == 8:
            landed(gain_plane, "zero_0", plane_send.at[1], plane_recv.at[1])
            for n in range(PLANE // 2):
                a, b = gain_plane[n // 2, n % 2 * 2], gain_plane[n // 2, n % 2 * 2 + 1]
                five = [a[:, :128], a[:, 128:256], a[:, 256:] + b[:, :128], b[:, 128:256], b[:, 256:]]
                for j in range(5):
                    gain_rows[n * 5 + j : n * 5 + j + 1, :] = five[j]
            gain[...] = gain_rows[...].astype(jnp.bfloat16)
        return []

    pl.when(z < top)(lambda: pl.semaphore_wait(ready, 2 - lower))
    sent += gains_at(0)
    for k in range(len(ORDER)):
        for link in range(4):
            copy(link, k, True).wait_recv()
        sent += gains_at(k + 1)
        for link in range(4):
            if k in NEXT:
                copy(link, NEXT[k], False).start()
    for c in sent:
        c.wait_send()
    for step, up in hops:
        hop(step, up, False).wait_send()
    for link in range(4):
        for half in range(2):
            early_copy(link, half).wait_send()
        for k in range(len(ORDER)):
            copy(link, k, False).wait_send()


def store(out, result, scale_q, scale_k, scale_v, gain, *rest):
    finals, scales, serve, results, sem = rest[0:3], rest[3:6], rest[6], rest[7:10], rest[10]
    width = finals[0].shape[-1]
    copies = []
    for w, scale in enumerate((scale_q, scale_k, scale_v)):
        columns = slice(w * width, (w + 1) * width)
        for part in range(2):
            at = pl.ds(part * SIDE // 2, SIDE // 2)
            copies.append((out.at[at, :, :, :, columns], finals[w].at[at]))
        copies.append((result.at[:, columns], results[w]))
        copies.append((scale, scales[w]))
    copies.append((gain, serve))
    started = [pltpu.make_async_copy(a, b, sem.at[n]) for n, (a, b) in enumerate(copies)]
    for c in started:
        c.start()
    for c in started:
        c.wait()


def body(*args):
    rows, width = args[0].shape
    f32, bf16 = jnp.float32, jnp.bfloat16
    hbm, vmem = pl.BlockSpec(memory_space=pltpu.HBM), pl.BlockSpec(memory_space=pltpu.VMEM)
    dma = pltpu.SemaphoreType.DMA
    gains = args[6].shape[0] * DEPTH * PLANE
    steps = len(ORDER)
    unit = rows // 4
    most = max(sum(v) for v in EARLY.values())
    args = [pltpu.with_memory_space_constraint(a, pltpu.HBM) for a in (*args[:6], args[6][None], args[7][None])]
    held = pl.pallas_call(
        work,
        out_shape=(
            pltpu.VMEM((SIDE, SIDE, 4, unit, 3 * width), bf16),
            pltpu.VMEM((rows, 3 * width), f32),
            *[pltpu.VMEM((width,), f32)] * 3,
            pltpu.VMEM((gains // 128, 128), bf16),
        ),
        in_specs=[hbm] * 8,
        out_specs=(vmem,) * 6,
        scratch_shapes=[
            pltpu.VMEM((rows, 3 * width), f32),
            pltpu.VMEM((rows, 3 * width), f32),
            pltpu.VMEM((4, most, 3 * width), f32),
            pltpu.VMEM((SIDE + 1, 1, 3 * width), f32),
            pltpu.VMEM((SIDE + 1, 1, 3 * width), f32),
            pltpu.VMEM((2 + 8, 1, args[6].shape[1]), f32),
            pltpu.VMEM((DEPTH + 3, 1, WINDOW), f32),
            pltpu.VMEM((SIDE + 1, SIDE, 1, WINDOW), f32),
            pltpu.VMEM((gains // 128, 128), f32),
            dma((8, 3, 2)), dma((2,)),
            dma((4, 2)), dma((4, 2)),
            dma((2, 3)), dma((2, 3)),
            dma((7,)), dma((7,)),
            dma((2, 3)), dma((2, 3)),
            dma((4, steps)), dma((4, steps)),
            pltpu.SemaphoreType.REGULAR,
        ],
        compiler_params=pltpu.CompilerParams(
            collective_id=0, has_side_effects=True, vmem_limit_bytes=20 << 20
        ),
        name="gather",
    )(*args)
    outs = pl.pallas_call(
        store,
        out_shape=(
            *[jax.ShapeDtypeStruct((SIDE, SIDE, 4, unit, width), bf16)] * 3,
            *[jax.ShapeDtypeStruct((width,), f32)] * 3,
            jax.ShapeDtypeStruct((gains // 128, 128), bf16),
            *[jax.ShapeDtypeStruct((rows, width), f32)] * 3,
        ),
        in_specs=[vmem] * 6,
        out_specs=(hbm,) * 10,
        scratch_shapes=[dma((13,))],
        compiler_params=pltpu.CompilerParams(vmem_limit_bytes=2 << 20),
        name="store",
    )(*held)
    finals = [f.reshape(PLANE * rows, width) for f in outs[:3]]
    return (*finals, *outs[3:6], outs[6].reshape(gains), *outs[7:])


def solution(mesh):
    torus = Mesh(
        mesh.devices.reshape(SIDE, SIDE, mesh.shape["model"], mesh.shape["copy"]),
        ("zero_0", "zero_1", "model", "copy"),
    )
    weight, whole = P(COPY_ZERO, "model"), P("copy", "model")
    return jax.shard_map(
        body,
        mesh=torus,
        in_specs=(weight,) * 6 + (P(COPY_ZERO_MODEL),) * 2,
        out_specs=(whole,) * 3 + (P(("copy", "model")),) * 3 + (P("copy"),) + (weight,) * 3,
        check_vma=False,
    )
```

```python
import functools

import jax
import jax.numpy as jnp
from jax import lax
from jax.experimental import pallas as pl
from jax.experimental.pallas import tpu as pltpu
from jax.sharding import Mesh
from jax.sharding import PartitionSpec as P

COPY_ZERO = ("copy", "zero_0", "zero_1")
COPY_ZERO_MODEL = ("copy", "zero_0", "zero_1", "model")
MESH = pl.DeviceIdType.MESH

KEEP_RATE = 0.75
SIDE = 4
PLANE = SIDE * SIDE
DEPTH = 8
LINKS = (("zero_1", 1), ("zero_1", -1), ("zero_0", 1), ("zero_0", -1))
WINDOW = 384
EARLY = {"zero_1": (8, 32), "zero_0": (24, 16)}


ORDER = (
    ("own 1", None), ("own 0", None), ("side 1", 0), ("pass", None), ("side 1", -1), ("side 1", 1), ("side 1", 2),
    ("side 0", None), ("side pass", None),
)
FIRST = 3
NEXT = {0: 3, 1: 4, 2: 5, 3: 6, 4: 7, 6: 8}


def place(here, link, kind, across, arrived):
    axis, step = LINKS[link]
    along = (-step if "pass" in kind else 0) - (step if arrived else 0)
    at = lax.rem(here[axis] + along + 2 * SIDE, SIDE)
    if "side" in kind:
        unit = link ^ 2 if kind != "side 0" else link ^ 3
        other = "zero_0" if axis == "zero_1" else "zero_1"
        beside = slice(None) if across is None else lax.rem(here[other] + across + SIDE, SIDE)
        return (beside, at, unit) if axis == "zero_1" else (at, beside, unit)
    unit = link ^ 1 if kind == "own 0" else link
    return (here["zero_0"], at, unit) if axis == "zero_1" else (at, here["zero_1"], unit)


def work(
    train_q, slow_q, train_k, slow_k, train_v, slow_v, gain_train, gain_step,
    out, result, scale_q, scale_k, scale_v, gain,
    train, slow, early, sums_x, sums_y, gains, gain_z, gain_plane, gain_rows,
    load_sem, gain_sem, early_send, early_recv, sum_send, sum_recv, z_send, z_recv, plane_send, plane_recv,
    link_send, link_recv, ready,
):
    rows, width = train_q.shape
    unit = rows // 4
    columns = [slice(w * width, (w + 1) * width) for w in range(3)]
    x, y, z = lax.axis_index("zero_1"), lax.axis_index("zero_0"), lax.axis_index("model")
    me = y * SIDE + x
    here = {"zero_1": x, "zero_0": y}

    def near(axis, step):
        return {axis: lax.rem(here[axis] + step + SIDE, SIDE)}

    def deep(step):
        return lax.rem(z + step + DEPTH, DEPTH)

    barrier = pltpu.get_barrier_semaphore()
    friends = [near(axis, step) for axis in ("zero_1", "zero_0") for step in (1, 2, 3)]
    for friend in friends:
        pl.semaphore_signal(barrier, inc=1, device_id=friend, device_id_type=MESH)

    top = DEPTH - 1
    lower = (z + top) // DEPTH + (z + 1) // DEPTH

    def greet(sem, step):
        pl.semaphore_signal(sem, inc=1, device_id={"model": deep(step)}, device_id_type=MESH)

    pl.when(z < top)(lambda: greet(barrier, 1))
    pl.when(z == 0)(lambda: greet(barrier, -1))

    ahead = [sum(EARLY[axis]) for axis, _ in LINKS]
    first = [EARLY[axis][0] for axis, _ in LINKS]
    spans = [(u * unit, first[u]) for u in range(4)] + [(u * unit + first[u], unit - first[u]) for u in range(4)]
    loads = []
    for n, (start, size) in enumerate(spans):
        at = pl.ds(start, size)
        group = []
        for w, (t, s) in enumerate(((train_q, slow_q), (train_k, slow_k), (train_v, slow_v))):
            group.append(pltpu.make_async_copy(t.at[at, :], train.at[at, columns[w]], load_sem.at[n, w, 0]))
            group.append(pltpu.make_async_copy(s.at[at, :], slow.at[at, columns[w]], load_sem.at[n, w, 1]))
        for c in group:
            c.start()
        loads.append(group)
    gain_loads = [
        pltpu.make_async_copy(gain_train, gains.at[0], gain_sem.at[0]),
        pltpu.make_async_copy(gain_step, gains.at[1], gain_sem.at[1]),
    ]
    for c in gain_loads:
        c.start()

    def average(n):
        for c in loads[n]:
            c.wait()
        start, size = spans[n]
        r = KEEP_RATE * slow[start : start + size, :] + (1.0 - KEEP_RATE) * train[start : start + size, :]
        result[start : start + size, :] = r
        return jnp.sum((r * r).reshape(size // 8, 8, 3 * width), axis=0)

    def early_copy(link, half):
        axis, step = LINKS[link]
        first, second = EARLY[axis]
        start, size = (0, first) if half == 0 else (first, second)
        return pltpu.make_async_remote_copy(
            src_ref=result.at[pl.ds(link * unit + start, size), :], dst_ref=early.at[link, pl.ds(start, size), :],
            send_sem=early_send.at[link, half], recv_sem=early_recv.at[link, half],
            device_id=near(axis, step), device_id_type=MESH,
        )

    square = average(0)
    for n in range(1, 4):
        square = square + average(n)
    pl.semaphore_wait(barrier, len(friends) + lower)
    for link in range(4):
        early_copy(link, 0).start()
    for n in range(4, 8):
        square = square + average(n)

    def ring(ref, index, axis, send, recv):
        copies = []
        for step in (1, 2, 3):
            copies.append(pltpu.make_async_remote_copy(
                src_ref=ref.at[index], dst_ref=ref.at[index], send_sem=send.at[step - 1], recv_sem=recv.at[step - 1],
                device_id=near(axis, step), device_id_type=MESH,
            ))
            copies[-1].start()
        return copies

    def landed(ref, axis, send, recv):
        for step in (1, 2, 3):
            index = near(axis, -step)[axis]
            pltpu.make_async_remote_copy(
                src_ref=ref.at[index], dst_ref=ref.at[index], send_sem=send.at[step - 1], recv_sem=recv.at[step - 1],
                device_id=near(axis, step), device_id_type=MESH,
            ).wait_recv()

    sums_x[x] = jnp.sum(square, axis=0, keepdims=True)
    sent = ring(sums_x, x, "zero_1", sum_send.at[0], sum_recv.at[0])
    for link in (0, 1):
        early_copy(link, 1).start()

    pl.when(z > 0)(lambda: greet(ready, -1))
    pl.when(z == top)(lambda: greet(ready, 1))

    for c in gain_loads:
        c.wait()
    value = (gains[0] + gains[1]).astype(jnp.bfloat16)
    count = gain_train.shape[1]
    put = (
        lax.broadcasted_iota(jnp.int32, (count, WINDOW), 1)
        == lax.broadcasted_iota(jnp.int32, (count, WINDOW), 0) + (lax.rem(me, 2) * 64 + z * count)
    )
    gain_z[z] = jnp.dot(value, jnp.where(put, 1.0, 0.0).astype(jnp.bfloat16), preferred_element_type=jnp.float32)

    landed(sums_x, "zero_1", sum_send.at[0], sum_recv.at[0])
    sums_y[y] = (sums_x[0] + sums_x[1]) + (sums_x[2] + sums_x[3])
    sent += ring(sums_y, y, "zero_0", sum_send.at[1], sum_recv.at[1])
    for link in (2, 3):
        early_copy(link, 1).start()
    landed(sums_y, "zero_0", sum_send.at[1], sum_recv.at[1])
    root = jnp.sqrt((sums_y[0] + sums_y[1]) + (sums_y[2] + sums_y[3]))
    inverse = 1.0 / root

    def normalise(link, start, size):
        out[y, x, link, pl.ds(start, size), :] = (
            result[link * unit + start : link * unit + start + size, :] * inverse
        ).astype(jnp.bfloat16)

    def piece(link, k, arrived):
        kind, across = ORDER[k]
        block = place(here, link, kind, across, arrived)
        start = ahead[link] if kind == "own 1" else 0
        return out.at[(*block, pl.ds(start, unit - start))]

    def copy(link, k, arrived):
        ref = piece(link, k, arrived)
        return pltpu.make_async_remote_copy(
            src_ref=ref, dst_ref=ref, send_sem=link_send.at[link, k], recv_sem=link_recv.at[link, k],
            device_id=near(*LINKS[link]), device_id_type=MESH,
        )

    for link in range(4):
        normalise(link, ahead[link], unit - ahead[link])
    for link in range(4):
        copy(link, 0, False).start()
    for link in range(4):
        normalise(link, 0, ahead[link])
    for k in range(1, FIRST):
        for link in range(4):
            copy(link, k, False).start()
    for w, ref in enumerate((scale_q, scale_k, scale_v)):
        ref[...] = root[0, columns[w]]

    for link in range(4):
        axis, step = LINKS[link]
        for half in range(2):
            early_copy(link, half).wait_recv()
        at = {**here, **near(axis, -step)}
        out[at["zero_0"], at["zero_1"], link, pl.ds(0, ahead[link]), :] = (
            early[link, : ahead[link], :] * inverse
        ).astype(jnp.bfloat16)

    def hop(step, up, arrived):
        index = deep((1 - step if up else step - 1) + (0 if not arrived else -1 if up else 1))
        at = (0 if up else 4) + step - 1
        return pltpu.make_async_remote_copy(
            src_ref=gain_z.at[index], dst_ref=gain_z.at[index], send_sem=z_send.at[at], recv_sem=z_recv.at[at],
            device_id={"model": deep(1 if up else -1)}, device_id_type=MESH,
        )

    hops = [(step, up) for step in range(1, 5) for up in ((True, False) if step < 4 else (True,))]

    def gains_at(k):
        if k <= 4:
            for step, up in hops:
                if step == k:
                    hop(step, up, True).wait_recv()
            for step, up in hops:
                if step == k + 1:
                    hop(step, up, False).start()
        if k == 4:
            column = gain_z[0]
            for n in range(1, DEPTH):
                column = column + gain_z[n]
            gain_plane[y, x] = column
            return ring(gain_plane.at[y], x, "zero_1", plane_send.at[0], plane_recv.at[0])
        if k == 6:
            landed(gain_plane.at[y], "zero_1", plane_send.at[0], plane_recv.at[0])
            return ring(gain_plane, y, "zero_0", plane_send.at[1], plane_recv.at[1])
        if k == 8:
            landed(gain_plane, "zero_0", plane_send.at[1], plane_recv.at[1])
            for n in range(PLANE // 2):
                a, b = gain_plane[n // 2, n % 2 * 2], gain_plane[n // 2, n % 2 * 2 + 1]
                five = [a[:, :128], a[:, 128:256], a[:, 256:] + b[:, :128], b[:, 128:256], b[:, 256:]]
                for j in range(5):
                    gain_rows[n * 5 + j : n * 5 + j + 1, :] = five[j]
            gain[...] = gain_rows[...].astype(jnp.bfloat16)
        return []

    pl.when(z < top)(lambda: pl.semaphore_wait(ready, 2 - lower))
    sent += gains_at(0)
    for k in range(len(ORDER)):
        for link in range(4):
            copy(link, k, True).wait_recv()
        sent += gains_at(k + 1)
        for link in range(4):
            if k in NEXT:
                copy(link, NEXT[k], False).start()
    for c in sent:
        c.wait_send()
    for step, up in hops:
        hop(step, up, False).wait_send()
    for link in range(4):
        for half in range(2):
            early_copy(link, half).wait_send()
        for k in range(len(ORDER)):
            copy(link, k, False).wait_send()


def store(out, result, scale_q, scale_k, scale_v, gain, *rest):
    finals, scales, serve, results, sem = rest[0:3], rest[3:6], rest[6], rest[7:10], rest[10]
    width = finals[0].shape[-1]
    copies = []
    for w, scale in enumerate((scale_q, scale_k, scale_v)):
        columns = slice(w * width, (w + 1) * width)
        for part in range(2):
            at = pl.ds(part * SIDE // 2, SIDE // 2)
            copies.append((out.at[at, :, :, :, columns], finals[w].at[at]))
        copies.append((result.at[:, columns], results[w]))
        copies.append((scale, scales[w]))
    copies.append((gain, serve))
    started = [pltpu.make_async_copy(a, b, sem.at[n]) for n, (a, b) in enumerate(copies)]
    for c in started:
        c.start()
    for c in started:
        c.wait()


def body(*args):
    rows, width = args[0].shape
    f32, bf16 = jnp.float32, jnp.bfloat16
    hbm, vmem = pl.BlockSpec(memory_space=pltpu.HBM), pl.BlockSpec(memory_space=pltpu.VMEM)
    dma = pltpu.SemaphoreType.DMA
    gains = args[6].shape[0] * DEPTH * PLANE
    steps = len(ORDER)
    unit = rows // 4
    most = max(sum(v) for v in EARLY.values())
    args = [pltpu.with_memory_space_constraint(a, pltpu.HBM) for a in (*args[:6], args[6][None], args[7][None])]
    held = pl.pallas_call(
        work,
        out_shape=(
            pltpu.VMEM((SIDE, SIDE, 4, unit, 3 * width), bf16),
            pltpu.VMEM((rows, 3 * width), f32),
            *[pltpu.VMEM((width,), f32)] * 3,
            pltpu.VMEM((gains // 128, 128), bf16),
        ),
        in_specs=[hbm] * 8,
        out_specs=(vmem,) * 6,
        scratch_shapes=[
            pltpu.VMEM((rows, 3 * width), f32),
            pltpu.VMEM((rows, 3 * width), f32),
            pltpu.VMEM((4, most, 3 * width), f32),
            pltpu.VMEM((SIDE + 1, 1, 3 * width), f32),
            pltpu.VMEM((SIDE + 1, 1, 3 * width), f32),
            pltpu.VMEM((2 + 8, 1, args[6].shape[1]), f32),
            pltpu.VMEM((DEPTH + 3, 1, WINDOW), f32),
            pltpu.VMEM((SIDE + 1, SIDE, 1, WINDOW), f32),
            pltpu.VMEM((gains // 128, 128), f32),
            dma((8, 3, 2)), dma((2,)),
            dma((4, 2)), dma((4, 2)),
            dma((2, 3)), dma((2, 3)),
            dma((7,)), dma((7,)),
            dma((2, 3)), dma((2, 3)),
            dma((4, steps)), dma((4, steps)),
            pltpu.SemaphoreType.REGULAR,
        ],
        compiler_params=pltpu.CompilerParams(
            collective_id=0, has_side_effects=True, vmem_limit_bytes=20 << 20
        ),
        name="gather",
    )(*args)
    outs = pl.pallas_call(
        store,
        out_shape=(
            *[jax.ShapeDtypeStruct((SIDE, SIDE, 4, unit, width), bf16)] * 3,
            *[jax.ShapeDtypeStruct((width,), f32)] * 3,
            jax.ShapeDtypeStruct((gains // 128, 128), bf16),
            *[jax.ShapeDtypeStruct((rows, width), f32)] * 3,
        ),
        in_specs=[vmem] * 6,
        out_specs=(hbm,) * 10,
        scratch_shapes=[dma((13,))],
        compiler_params=pltpu.CompilerParams(vmem_limit_bytes=2 << 20),
        name="store",
    )(*held)
    finals = [f.reshape(PLANE * rows, width) for f in outs[:3]]
    return (*finals, *outs[3:6], outs[6].reshape(gains), *outs[7:])


def solution(mesh):
    torus = Mesh(
        mesh.devices.reshape(SIDE, SIDE, mesh.shape["model"], mesh.shape["copy"]),
        ("zero_0", "zero_1", "model", "copy"),
    )
    weight, whole = P(COPY_ZERO, "model"), P("copy", "model")
    return jax.shard_map(
        body,
        mesh=torus,
        in_specs=(weight,) * 6 + (P(COPY_ZERO_MODEL),) * 2,
        out_specs=(whole,) * 3 + (P(("copy", "model")),) * 3 + (P("copy"),) + (weight,) * 3,
        check_vma=False,
    )
```
